128 devices in a mesh: dp: 8 (over z, core), mp: 16 (over y, x).
Axes of the slice: x: 4, y: 4, z: 4, core: 2. Of those that a mesh axis runs over, the one named last changes fastest.
Arguments:
- patches: bfloat16 [16384, 1280], P(('dp', 'mp')), may hold values from -6 to 6
- window_ids: int32 [128, 128], P(('dp', 'mp')), may hold values from 0 to 7, never falling along the last dimension, each value on 1 to 64 neighbouring positions
- owner: int32 [4096, 1], P(('dp', 'mp')), may hold values from 0 to 7; in each aligned block of 32 rows (0 to 31, 32 to 63, ...) at most 8 rows name the same one
- slot_of_row: int32 [128, 64], P(('dp', 'mp')), may hold values from 0 to 63, each once within a row
- text_embeds: bfloat16 [8192, 8192], P(('dp', 'mp')), may hold values from -6 to 6
- vit_norm: float32 [1280], replicated, may hold values from 0.3 to 3
- vit_qkv_w: bfloat16 [1280, 1920], replicated, may hold values from -0.15625 to 0.15625
- vit_qkv_b: float32 [1920], replicated, may hold values from -12 to 12
- vit_out_w: bfloat16 [640, 1280], replicated, may hold values from -0.25 to 0.25
- merge_norm: float32 [1280], replicated, may hold values from 0.3 to 3
- merge_w1: bfloat16 [5120, 5120], P(None, 'mp'), may hold values from -0.078125 to 0.078125
- merge_b1: float32 [5120], P('mp'), may hold values from -3 to 3
- merge_w2: bfloat16 [5120, 8192], P('mp'), may hold values from -0.078125 to 0.078125
- merge_b2: float32 [8192], replicated, may hold values from -3 to 3
- llm_norm: float32 [8192], replicated, may hold values from 0.5 to 1.5
- q_w: bfloat16 [8192, 4096], P(None, 'mp'), may hold values from -0.0625 to 0.0625
- q_b: float32 [4096], P('mp'), may hold values from -12 to 12
- kv_w: bfloat16 [2, 8192, 512], P(None, None, 'mp'), may hold values from -0.0625 to 0.0625
- kv_b: float32 [2, 512], P(None, 'mp'), may hold values from -12 to 12
Outputs:
- attended: bfloat16 [8192, 4096], P('dp', 'mp')
The draws below stay inside these ranges and needn't reach their ends.
Inputs may be any that keep to these rules, and one draw needn't show every extreme that they name: `window_ids`: within each block, window numbers never fall and each window has at most 64 patches. Among the 32 merged rows of one device, no owner is named by more than 8 rows, a bound that some block reaches. `slot_of_row`: each row is a permutation of the 64 slots.
All inputs are finite; a program needn't handle non-finite values.
Results may differ from the reference program's by a relative error of at most 0.04.
Values may be sent and summed in bfloat16 or wider, within the bound.
No kernel may reach another device: no remote copies, remote signals or barrier semaphores. Data moves between devices by JAX's collectives and lax.ppermute only.
A program may use at most 128 MiB of HBM per device.

```python
import math
import jax
import jax.numpy as jnp
import numpy as np
from jax import lax

VW = 1280
VHD = 80
VH = 8
D = 8192
HD = 128
QH = 32
KVH = 4
BLOCK = 128
ROWS_DEV = 64
MW = 5120
MR = 32
CAP = 8
SEQ = 1024
PATCHES = 16384
MERGED = 4096
TOTAL_ROWS = 8192
N_DP = 8
N_MP = 16
DEVICES = 128


def drawn_bias(key, bias_shape):
    return jnp.clip(0.5 * jax.random.normal(key, bias_shape, jnp.float32), -3.0, 3.0)


def draw_vit_qkv_b(key, part):
    noise_part = drawn_bias(jax.random.fold_in(key, 7201), (3, VH, VHD))
    return noise_part.reshape(3 * VH * VHD)


def draw_q_b(key, part):
    noise_part = drawn_bias(jax.random.fold_in(key, 7501), (QH, HD))
    return noise_part.reshape(QH * HD)


def draw_kv_b(key, part):
    noise_part = drawn_bias(jax.random.fold_in(key, 7601), (2, KVH, HD))
    return jnp.swapaxes(noise_part, 1, 2).reshape(2, KVH * HD)


def levels(key, shape, shards, least, high):
    factor_of, own = 1.0, jax.random.fold_in(key, 6)
    for axis_at, shards_of in shards:
        draws = jnp.exp(jax.random.uniform(jax.random.fold_in(own, axis_at), (shards_of,), jnp.float32, least / len(shards), high / len(shards)))
        factor_of = factor_of * jnp.repeat(draws, shape[axis_at] // shards_of).reshape([-1 if axis == axis_at else 1 for axis in range(len(shape))])
    return factor_of


def length_profile(number_of, total, limit, skew):
    loads = [(1 << 20) // math.isqrt(standing ** skew) + 1 for standing in range(2, number_of + 1)]
    spare, counts = total - limit - (number_of - 1), [1] * (number_of - 1)
    while spare > 0:
        movable = [i for i in range(number_of - 1) if counts[i] < limit]
        pool, budget = sum([loads[i] for i in movable]), spare
        for i in movable:
            extra = min(limit - counts[i], max(1, budget * loads[i] // pool), spare)
            counts[i] = counts[i] + extra
            spare = spare - extra
    return np.array([limit] + counts)


def uneven_parts(own_key, count, total, reach, skew):
    if count == 2:
        one = jax.random.randint(own_key, (), max(1, total - reach), min(reach, total - 1) + 1)
        return jnp.stack([one, total - one])
    tallies = jnp.asarray(length_profile(count, total, reach, skew), jnp.int32)
    couples = (count - 1) // 2
    donor, taker = tallies[1:1 + 2 * couples:2], tallies[2:2 + 2 * couples:2]
    room = jnp.minimum(donor - 1, reach - taker)
    passed = jax.random.randint(jax.random.fold_in(own_key, 1), (couples,), 0, 1 << 20) % (room + 1)
    tallies = tallies.at[1:1 + 2 * couples:2].set(donor - passed).at[2:2 + 2 * couples:2].set(taker + passed)
    return tallies[jax.random.permutation(jax.random.fold_in(own_key, 2), count)]


def shared_out(stream_key, own, number, rows, amount, top, limit, slope):
    ranking = jax.random.permutation(stream_key, amount)
    heavy_load, ordinary = shares(amount, rows * top, limit, slope, True), shares(amount, rows * top, limit, slope, False)
    places = jnp.arange(amount)

    def named(lengths, turn):
        used = int((lengths > 0).sum())
        fixed = max(1, used // 4)
        shifted = fixed + (places - fixed + turn * (used - fixed)) % max(1, amount - fixed)
        return jnp.zeros((amount,), jnp.int32).at[ranking[jnp.where(places < fixed, places, shifted)]].set(jnp.asarray(lengths, jnp.int32))

    lengths = jnp.where(number % 4 == 0, named(heavy_load, number // 4), named(ordinary, number - number // 4 - 1))
    mixed = jax.random.permutation(jax.random.fold_in(own, 3), amount)
    source_of, receiver = mixed[0:amount // 2 * 2:2], mixed[1:amount // 2 * 2:2]
    slack = jnp.minimum(lengths[source_of] - 1, limit - lengths[receiver]) // 2
    slack = jnp.where((source_of == ranking[0]) | (receiver == ranking[0]) | (lengths[receiver] == 0), 0, jnp.maximum(slack, 0))
    shifted = jax.random.randint(jax.random.fold_in(own, 4), (amount // 2,), 0, 1 << 20) % (slack + 1)
    lengths = lengths.at[source_of].add(-shifted).at[receiver].add(shifted)
    labels = jnp.searchsorted(jnp.cumsum(lengths), jnp.arange(rows * top), side="right").astype(jnp.int32)
    listing = labels.reshape(top, rows).T
    listing = listing[jax.random.permutation(jax.random.fold_in(own, 1), rows)]
    turn = jax.random.randint(jax.random.fold_in(own, 2), (rows, 1), 0, top)
    return jnp.take_along_axis(listing, (jnp.arange(top)[None, :] + turn) % top, axis=1)


def shares(count, total, limit, slope, full):
    portions = [(1 << 20) // math.isqrt(grade ** slope) + 1 for grade in range(1, count + 1)]
    largest = limit if full else min(limit, max(-(-total // count), total * portions[0] // sum(portions)))
    least = 1 if total - largest >= count - 1 else 0
    counts, rest = [largest] + [least] * (count - 1), total - largest - least * (count - 1)
    while rest > 0:
        candidates = [i for i in range(1, count) if counts[i] < largest] or [i for i in range(1, count) if counts[i] < limit]
        mass, left = sum([portions[i] for i in candidates]), rest
        for i in candidates:
            extra = min(limit - counts[i], max(1, left * portions[i] // mass), rest)
            counts[i] = counts[i] + extra
            rest = rest - extra
    return np.array(counts)


def centred(rng, shape, deviation, reach, cuts=(), kind=jnp.bfloat16):
    factor_of = levels(rng, shape, cuts, -0.22, 0.18) if cuts else 1.0
    array = jax.random.normal(rng, shape, jnp.float32) * deviation * factor_of
    return jnp.minimum(jnp.maximum(array, -reach), reach).astype(kind)


def setup_inputs(seed: int = 0) -> dict:
    keys = jax.random.split(jax.random.key(seed), 20)
    patches = centred(keys[0], (PATCHES, VW), 1.0, 6.0, ((0, 128),))
    window_ids = jax.vmap(lambda own: jnp.searchsorted(jnp.cumsum(uneven_parts(own, 8, BLOCK, BLOCK // 2, 2)), jnp.arange(BLOCK), side="right"))(jax.random.split(keys[1], (PATCHES // BLOCK))).reshape((PATCHES // BLOCK, BLOCK)).astype(jnp.int32)
    owner_keys = jax.random.split(jax.random.fold_in(keys[2], 1), MERGED // MR)
    owner_turns = jax.random.permutation(jax.random.fold_in(keys[2], 3), MERGED // MR)
    owner = jax.vmap(lambda own, number: shared_out(jax.random.fold_in(keys[2], 2), own, number, MR, N_DP, 1, CAP, 2))(owner_keys, owner_turns).reshape((MERGED, 1))
    slot_of_row = jax.vmap(lambda own: jax.random.permutation(own, ROWS_DEV))(jax.random.split(keys[3], DEVICES)).reshape((DEVICES, ROWS_DEV)).astype(jnp.int32)
    text_embeds = centred(keys[4], (TOTAL_ROWS, D), 1.0, 6.0, ((0, 128),))
    vit_norm = jnp.clip(jnp.exp(jax.random.uniform(keys[5], (VW,), jnp.float32, math.log(0.3), math.log(3.0))), 0.3, 3.0)
    vit_qkv_w = centred(keys[6], (VW, 3 * VH * VHD), VW ** -0.5, 0.15625)
    vit_qkv_b = draw_vit_qkv_b(jax.random.fold_in(keys[19], 71), 0)
    vit_out_w = centred(keys[8], (VH * VHD, VW), (VH * VHD) ** -0.5, 0.25)
    merge_norm = jnp.clip(jnp.exp(jax.random.uniform(keys[9], (VW,), jnp.float32, math.log(0.3), math.log(3.0))), 0.3, 3.0)
    merge_w1 = centred(keys[10], (MW, MW), MW ** -0.5, 0.078125, ((1, 16),))
    merge_b1 = centred(keys[11], (MW,), 0.5, 3.0, ((0, 16),), jnp.float32)
    merge_w2 = centred(keys[12], (MW, D), MW ** -0.5, 0.078125, ((0, 16),))
    merge_b2 = centred(keys[13], (D,), 0.5, 3.0, (), jnp.float32)
    llm_norm = jnp.clip(1.0 + 0.1 * jax.random.normal(keys[14], (D,), jnp.float32), 0.5, 1.5)
    q_w = centred(keys[15], (D, QH * HD), D ** -0.5, 0.0625, ((1, 16),))
    q_b = draw_q_b(jax.random.fold_in(keys[19], 71), 0)
    kv_w = centred(keys[17], (2, D, KVH * HD), D ** -0.5, 0.0625, ((2, 16),))
    kv_b = draw_kv_b(jax.random.fold_in(keys[19], 71), 0)
    return dict(patches=patches, window_ids=window_ids, owner=owner, slot_of_row=slot_of_row, text_embeds=text_embeds, vit_norm=vit_norm, vit_qkv_w=vit_qkv_w, vit_qkv_b=vit_qkv_b, vit_out_w=vit_out_w, merge_norm=merge_norm, merge_w1=merge_w1, merge_b1=merge_b1, merge_w2=merge_w2, merge_b2=merge_b2, llm_norm=llm_norm, q_w=q_w, q_b=q_b, kv_w=kv_w, kv_b=kv_b)


epsilon = 1e-06

def rms_norm(inputs, gain):
    inputs = inputs.astype(jnp.float32)
    return inputs * lax.rsqrt(lax.optimization_barrier(jnp.mean(inputs * inputs, axis=-1, keepdims=True)) + epsilon) * gain

def vision_block(patches, window_ids, vit_norm, vit_qkv_w, vit_qkv_b, vit_out_w, merge_norm):
    normed = rms_norm(patches, vit_norm).astype(jnp.bfloat16)
    projected = (jnp.dot(normed, vit_qkv_w, preferred_element_type=jnp.float32) + vit_qkv_b).astype(jnp.bfloat16)
    blocks = window_ids.shape[0]
    width = window_ids.shape[1]
    inner_width = vit_out_w.shape[0]
    heads = inner_width // VHD
    shaped = projected.reshape(blocks, width, 3, heads, VHD).astype(jnp.float32)
    scores = jnp.einsum('bqhd,bkhd->bhqk', shaped[:, :, 0], shaped[:, :, 1]) * VHD ** (-0.5)
    in_window = window_ids[:, None, :, None] == window_ids[:, None, None, :]
    scores = jnp.where(in_window, scores, -1e+30)
    peak = lax.optimization_barrier(jnp.max(scores, axis=-1, keepdims=True))
    weights = jnp.exp(scores - peak)
    weights = (weights / lax.optimization_barrier(jnp.sum(weights, axis=-1, keepdims=True))).astype(jnp.bfloat16)
    mixture = jnp.einsum('bhqk,bkhd->bqhd', weights.astype(jnp.float32), shaped[:, :, 2])
    mixture = mixture.astype(jnp.bfloat16).reshape(blocks * width, inner_width)
    residual = (patches.astype(jnp.float32) + jnp.dot(mixture, vit_out_w, preferred_element_type=jnp.float32)).astype(jnp.bfloat16)
    merged = rms_norm(residual, merge_norm).astype(jnp.bfloat16)
    return merged.reshape(blocks * width // 4, 4 * patches.shape[1])

def causal_heads(queries, key_heads, value_heads):
    length = queries.shape[0]
    scores = jnp.einsum('qhd,khd->hqk', queries.astype(jnp.float32), key_heads.astype(jnp.float32)) * HD ** (-0.5)
    allowed = jnp.arange(length)[:, None] >= jnp.arange(length)[None, :]
    scores = jnp.where(allowed[None], scores, -1e+30)
    peak = lax.optimization_barrier(jnp.max(scores, axis=-1, keepdims=True))
    weights = jnp.exp(scores - peak)
    weights = (weights / lax.optimization_barrier(jnp.sum(weights, axis=-1, keepdims=True))).astype(jnp.bfloat16)
    mixture = jnp.einsum('hqk,khd->qhd', weights.astype(jnp.float32), value_heads.astype(jnp.float32))
    return mixture.astype(jnp.bfloat16).reshape(length, -1)

def reference(patches, window_ids, owner, slot_of_row, text_embeds, vit_norm, vit_qkv_w, vit_qkv_b, vit_out_w, merge_norm, merge_w1, merge_b1, merge_w2, merge_b2, llm_norm, q_w, q_b, kv_w, kv_b):
    merged = vision_block(patches, window_ids, vit_norm, vit_qkv_w, vit_qkv_b, vit_out_w, merge_norm)
    hidden = jax.nn.gelu(jnp.dot(merged, merge_w1, preferred_element_type=jnp.float32) + merge_b1, approximate=False).astype(jnp.bfloat16)
    shard_width = MW // N_MP

    def add_shard(running, shard_index):
        first = shard_index * shard_width
        part_hidden = lax.dynamic_slice_in_dim(hidden, first, shard_width, 1)
        part_weight = lax.dynamic_slice_in_dim(merge_w2, first, shard_width, 0)
        partial_value = jnp.dot(part_hidden, part_weight, preferred_element_type=jnp.float32)
        rounded = lax.optimization_barrier(partial_value.astype(jnp.bfloat16))
        return (running + rounded.astype(jnp.float32), 0)
    start_sum = jnp.zeros((merged.shape[0], D), jnp.float32)
    running, unused = lax.scan(add_shard, start_sum, jnp.arange(N_MP, dtype=jnp.int32))
    embedded = (running + merge_b2).astype(jnp.bfloat16)
    devices = DEVICES
    row_ids = jnp.arange(MERGED, dtype=jnp.int32)
    sender = row_ids // MR
    sender_dp = sender // N_MP
    sender_mp = sender % N_MP
    target_group = owner[:, 0]
    onehot = (target_group[:, None] == jnp.arange(N_DP, dtype=jnp.int32)[None, :]).astype(jnp.int32)
    per_device = onehot.reshape(devices, MR, N_DP)
    earlier = (jnp.cumsum(per_device, axis=1) - per_device).reshape(MERGED, N_DP)
    rank_in = lax.optimization_barrier(jnp.sum(earlier * onehot, axis=1))
    target_device = target_group * N_MP + sender_mp
    global_slot = (target_device * ROWS_DEV + sender_dp * CAP + rank_in).astype(jnp.int32)
    buffer = jnp.zeros((TOTAL_ROWS, D), jnp.bfloat16).at[global_slot].set(embedded)
    filled = jnp.zeros((TOTAL_ROWS,), jnp.int32).at[global_slot].set(1)
    source_rows = (jnp.arange(devices, dtype=jnp.int32)[:, None] * ROWS_DEV + slot_of_row).reshape(-1).astype(jnp.int32)
    sequence = jnp.where(filled[source_rows][:, None] > 0, buffer[source_rows], text_embeds)
    llm_normed = rms_norm(sequence, llm_norm).astype(jnp.bfloat16)
    queries = (jnp.dot(llm_normed, q_w, preferred_element_type=jnp.float32) + q_b).astype(jnp.bfloat16)
    key_rows = (jnp.dot(llm_normed, kv_w[0], preferred_element_type=jnp.float32) + kv_b[0]).astype(jnp.bfloat16)
    value_rows = (jnp.dot(llm_normed, kv_w[1], preferred_element_type=jnp.float32) + kv_b[1]).astype(jnp.bfloat16)
    group_size = QH // KVH

    def one_group(inputs):
        group_queries, group_keys, group_values = inputs
        key_heads = jnp.repeat(jnp.swapaxes(group_keys, 1, 2), group_size, axis=1)
        value_heads = jnp.repeat(jnp.swapaxes(group_values, 1, 2), group_size, axis=1)
        return causal_heads(group_queries, key_heads, value_heads)
    attended = lax.map(one_group, (queries.reshape(N_DP, SEQ, QH, HD), key_rows.reshape(N_DP, SEQ, HD, KVH), value_rows.reshape(N_DP, SEQ, HD, KVH)))
    return attended.reshape(N_DP * SEQ, QH * HD)
```

```python
import jax
import jax.numpy as jnp
from jax import lax
from jax.experimental import pallas as pl
from jax.experimental.pallas import tpu as pltpu
from jax.sharding import PartitionSpec as P

VHD = 80
HD = 128
KVH = 4


epsilon = 1e-06


def rms_norm(inputs, gain):
    inputs = inputs.astype(jnp.float32)
    return inputs * lax.rsqrt(jnp.mean(inputs * inputs, axis=-1, keepdims=True) + epsilon) * gain


def vision_block(patches, window_ids, vit_norm, vit_qkv_w, vit_qkv_b, vit_out_w, merge_norm):
    normed = rms_norm(patches, vit_norm).astype(jnp.bfloat16)
    projected = (jnp.dot(normed, vit_qkv_w, preferred_element_type=jnp.float32) + vit_qkv_b).astype(
        jnp.bfloat16
    )
    blocks = window_ids.shape[0]
    width = window_ids.shape[1]
    inner_width = vit_out_w.shape[0]
    heads = inner_width // VHD
    shaped = projected.reshape(blocks, width, 3, heads, VHD)
    scores = jnp.einsum(
        "bqhd,bkhd->bhqk", shaped[:, :, 0], shaped[:, :, 1], preferred_element_type=jnp.float32
    ) * VHD ** (-0.5)
    in_window = window_ids[:, None, :, None] == window_ids[:, None, None, :]
    scores = jnp.where(in_window, scores, -1e30)
    peak = jnp.max(scores, axis=-1, keepdims=True)
    weights = jnp.exp(scores - peak)
    weights = (weights / jnp.sum(weights, axis=-1, keepdims=True)).astype(jnp.bfloat16)
    mixture = jnp.einsum(
        "bhqk,bkhd->bqhd", weights, shaped[:, :, 2], preferred_element_type=jnp.float32
    )
    mixture = mixture.astype(jnp.bfloat16).reshape(blocks * width, inner_width)
    residual = (
        patches.astype(jnp.float32)
        + jnp.dot(mixture, vit_out_w, preferred_element_type=jnp.float32)
    ).astype(jnp.bfloat16)
    merged = rms_norm(residual, merge_norm).astype(jnp.bfloat16)
    return merged.reshape(blocks * width // 4, 4 * patches.shape[1])


def shards(
    patches,
    window_ids,
    owner,
    slot_of_row,
    text_embeds,
    vit_norm,
    vit_qkv_w,
    vit_qkv_b,
    vit_out_w,
    merge_norm,
    merge_w1,
    merge_b1,
    merge_w2,
    merge_b2,
    llm_norm,
    q_w,
    q_b,
    kv_w,
    kv_b,
):
    merged = vision_block(
        patches, window_ids, vit_norm, vit_qkv_w, vit_qkv_b, vit_out_w, merge_norm
    )
    rows_all = lax.all_gather(merged, "mp", axis=0, tiled=True)
    hidden = jax.nn.gelu(
        jnp.dot(rows_all, merge_w1, preferred_element_type=jnp.float32) + merge_b1,
        approximate=False,
    ).astype(jnp.bfloat16)
    own_rows = lax.psum_scatter(
        jnp.dot(hidden, merge_w2, preferred_element_type=jnp.float32).astype(jnp.bfloat16),
        "mp",
        scatter_dimension=0,
        tiled=True,
    ).astype(jnp.float32)
    embedded = (own_rows + merge_b2).astype(jnp.bfloat16)
    seq_rows = text_embeds.shape[0]
    groups = lax.axis_size("dp")
    capacity = seq_rows // groups
    target_group = owner[:, 0]
    onehot = (target_group[:, None] == jnp.arange(groups, dtype=jnp.int32)[None, :]).astype(
        jnp.int32
    )
    rank_in = jnp.sum((jnp.cumsum(onehot, axis=0) - onehot) * onehot, axis=1)
    send_slot = target_group * capacity + rank_in
    selector = send_slot[None, :] == jnp.arange(seq_rows, dtype=jnp.int32)[:, None]
    buffer = jnp.dot(
        selector.astype(jnp.bfloat16), embedded, preferred_element_type=jnp.float32
    ).astype(jnp.bfloat16)
    buffer = buffer.reshape(groups, capacity, embedded.shape[1])
    marks = jnp.sum(selector.astype(jnp.int32), axis=1).reshape(groups, capacity)
    arrived, arrived_marks = (
        lax.all_to_all(buffer, "dp", split_axis=0, concat_axis=0, tiled=True),
        lax.all_to_all(marks, "dp", split_axis=0, concat_axis=0, tiled=True),
    )
    arrived = arrived.reshape(seq_rows, embedded.shape[1])
    arrived_marks = arrived_marks.reshape(seq_rows)
    chosen = slot_of_row[0]
    sequence = jnp.where(arrived_marks[chosen][:, None] > 0, arrived[chosen], text_embeds)
    llm_normed = rms_norm(sequence, llm_norm).astype(jnp.bfloat16)
    kv_cols = kv_w.shape[2]
    shard_rows = lax.all_gather(llm_normed, "mp", axis=0, tiled=True)
    queries = (jnp.dot(shard_rows, q_w, preferred_element_type=jnp.float32) + q_b).astype(
        jnp.bfloat16
    )
    length = shard_rows.shape[0]
    kv_rows = lax.dot_general(
        kv_w, shard_rows, (((1,), (1,)), ((), ())), preferred_element_type=jnp.float32
    )
    kv_rows = (kv_rows + kv_b[:, :, None]).astype(jnp.bfloat16)
    shards_mp = lax.axis_size("mp")
    dims_here = kv_cols // KVH
    by_head = jnp.swapaxes(kv_rows.reshape(2, dims_here, KVH, length), 1, 2)
    for_each = jnp.broadcast_to(
        by_head[:, :, None], (2, KVH, shards_mp // KVH, dims_here, length)
    ).reshape(2, shards_mp, dims_here, length)
    own_head = lax.all_to_all(for_each, "mp", 1, 1, tiled=True).reshape(2, HD, length)
    return attention(queries, own_head[0], own_head[1])


def attention_kernel(queries_ref, keys_ref, values_ref, out_ref):
    length, cols = queries_ref.shape
    block = 256
    scale = HD ** (-0.5)
    row = lax.broadcasted_iota(jnp.int32, (block, block), 0)
    col = lax.broadcasted_iota(jnp.int32, (block, block), 1)
    allowed = row >= col
    for head in range(cols // HD):
        lanes = slice(head * HD, (head + 1) * HD)
        for first in range(0, length, block):
            last = first + block
            own = queries_ref[first:last, lanes]
            diagonal = jnp.dot(
                own, keys_ref[:, first:last], preferred_element_type=jnp.float32
            )
            diagonal = jnp.where(allowed, diagonal, -1e30)
            peak = jnp.max(diagonal, axis=-1, keepdims=True)
            if first:
                before = jnp.dot(own, keys_ref[:, :first], preferred_element_type=jnp.float32)
                peak = jnp.maximum(peak, jnp.max(before, axis=-1, keepdims=True))
            weights = jnp.exp((diagonal - peak) * scale)
            total = jnp.sum(weights, axis=-1, keepdims=True)
            mixed = lax.dot_general(
                weights.astype(jnp.bfloat16),
                values_ref[:, first:last],
                (((1,), (1,)), ((), ())),
                preferred_element_type=jnp.float32,
            )
            if first:
                weights = jnp.exp((before - peak) * scale)
                total = total + jnp.sum(weights, axis=-1, keepdims=True)
                mixed = mixed + lax.dot_general(
                    weights.astype(jnp.bfloat16),
                    values_ref[:, :first],
                    (((1,), (1,)), ((), ())),
                    preferred_element_type=jnp.float32,
                )
            out_ref[first:last, lanes] = (mixed / total).astype(jnp.bfloat16)


def attention(queries, keys, values):
    return pl.pallas_call(
        attention_kernel,
        out_shape=jax.ShapeDtypeStruct(queries.shape, jnp.bfloat16),
        name="causal_attention",
    )(queries, keys, values)


def solution(mesh):
    return jax.shard_map(
        shards,
        mesh=mesh,
        in_specs=(
            P(("dp", "mp"), None),
            P(("dp", "mp"), None),
            P(("dp", "mp"), None),
            P(("dp", "mp"), None),
            P(("dp", "mp"), None),
            P(),
            P(),
            P(),
            P(),
            P(),
            P(None, "mp"),
            P("mp"),
            P("mp", None),
            P(),
            P(),
            P(None, "mp"),
            P("mp"),
            P(None, None, "mp"),
            P(None, "mp"),
        ),
        out_specs=P("dp", "mp"),
        check_vma=False,
    )
```
